256 devices in a mesh: high: 16 (over z, core), low: 16 (over y, x).
Axes of the slice: x: 4, y: 4, z: 8, core: 2. Of those that a mesh axis runs over, the one named last changes fastest.
Arguments:
- wave_parts: float32 [2, 1024, 128, 128], P(None, ('high', 'low')), may hold values from -6 to 6
- level_table: float32 [1024, 128, 128], P(('high', 'low')), may hold values from -2 to 2
- phase_angles: float32 [2, 128], replicated, may hold values from 0.3 to 1.2
- mix_angles: float32 [2, 4], replicated, may hold values from 0.3 to 1.2
Outputs:
- result_parts: float32 [2, 1024, 128, 128], P(None, ('high', 'low'))
- marginal: float32 [64, 128, 128], P('low', 'high')
The draws below stay inside these ranges and needn't reach their ends.
All inputs are finite; a program needn't handle non-finite values.
Results may differ from the reference program's by a relative error of at most 0.0003.
Values sent between devices are 32-bit elements; how exact they have to be, the bound alone decides.
A program may use at most 64 MiB of HBM per device.

```python
import jax
import jax.numpy as jnp
from jax import lax

BLOCKS_DEV = 4
ROWS = 128
LANES = 128
BLOCKS = 1024
LAYERS = 2
N_HIGH = 16
N_LOW = 16


def block_scale(stream_key, extent, cuts, least, high):
    factor_of = 1.0
    for dim, blocks in cuts:
        heights = jax.random.uniform(jax.random.fold_in(jax.random.fold_in(stream_key, 6), dim), (blocks,), jnp.float32, least / len(cuts), high / len(cuts))
        factor_of = factor_of * jnp.repeat(jnp.exp(heights), extent[dim] // blocks).reshape((-1,) + (1,) * (len(extent) - 1 - dim))
    return factor_of


def normal_values(key, extent, deviation, most, split=(), kind=jnp.bfloat16):
    level = block_scale(key, extent, split, -0.22, 0.18) if split else 1.0
    values = jax.random.normal(key, extent, jnp.float32) * deviation * level
    return jnp.minimum(jnp.maximum(values, -most), most).astype(kind)


def setup_inputs(seed: int = 0) -> dict:
    streams_of = jax.random.split(jax.random.key(seed), 5)
    wave_parts = normal_values(streams_of[0], (2, BLOCKS, ROWS, LANES), 1.0, 6.0, ((1, 256),), jnp.float32)
    level_table = jnp.clip(jax.random.uniform(streams_of[1], (BLOCKS, ROWS, LANES), jnp.float32, -2.0, 2.0) * block_scale(streams_of[1], (BLOCKS, ROWS, LANES), ((0, 256),), -0.4, 0.0), -2.0, 2.0)
    phase_angles = jnp.clip(jax.random.uniform(streams_of[2], (LAYERS, LANES), jnp.float32, 0.3, 1.2), 0.3, 1.2)
    mix_angles = jnp.clip(jax.random.uniform(streams_of[3], (LAYERS, 4), jnp.float32, 0.3, 1.2), 0.3, 1.2)
    return dict(wave_parts=wave_parts, level_table=level_table, phase_angles=phase_angles, mix_angles=mix_angles)


def count_bits(values, count):
    places = jnp.arange(count.bit_length() - 1, dtype=jnp.int32)
    return jnp.sum((values[..., None] >> places) & 1, axis=-1)


def real_turn_table(count, angle):
    rank = jnp.arange(count, dtype=jnp.int32)
    apart = count_bits(rank[:, None] ^ rank[None, :], count)
    minus = count_bits(rank[:, None] & (rank[:, None] ^ rank[None, :]), count)
    bits = count.bit_length() - 1
    size = jnp.cos(angle) ** (bits - apart).astype(jnp.float32) * jnp.sin(angle) ** apart.astype(jnp.float32)
    return size * jnp.where(minus % 2 == 1, -1.0, 1.0).astype(jnp.float32)


def apply_along(values, dim, angle):
    real_part = real_turn_table(values.shape[dim], angle)
    def times(table):
        moved = jnp.tensordot(values, table, axes=([dim], [0]), precision=lax.Precision.HIGHEST)
        return jnp.moveaxis(moved, -1, dim)
    return times(real_part)


def phase_step(values, levels, angle):
    turn = angle * levels
    return jnp.stack([values[0] * jnp.cos(turn) + values[1] * jnp.sin(turn), values[1] * jnp.cos(turn) - values[0] * jnp.sin(turn)])


def reference(wave_parts, level_table, phase_angles, mix_angles):
    values = wave_parts
    for layer in range(LAYERS):
        values = phase_step(values, level_table, phase_angles[layer])
        values = apply_along(values, 3, mix_angles[layer, 0])
        values = apply_along(values, 2, mix_angles[layer, 1])
        parts = values.reshape(2, N_HIGH, N_LOW, BLOCKS_DEV, ROWS, LANES)
        parts = apply_along(parts, 1, mix_angles[layer, 2])
        parts = apply_along(parts, 2, mix_angles[layer, 3])
        parts = apply_along(parts, 3, mix_angles[layer, 2])
        values = parts.reshape(values.shape)
    chance = values[0] * values[0] + values[1] * values[1]
    marginal = jnp.mean(chance.reshape(N_HIGH, -1, ROWS, LANES), axis=0)
    return values, marginal
```

```python
import functools

import jax
import jax.numpy as jnp
import numpy as np
from jax import lax
from jax.experimental import pallas as pl
from jax.experimental.pallas import tpu as pltpu
from jax.sharding import PartitionSpec as P

MESH = pl.DeviceIdType.MESH
T = 4
SUB, LANES = 8, 128
F32 = jnp.float32


def even_series(fn, terms, most):
    k = np.arange(4 * terms)
    y = (np.cos((k + 0.5) * np.pi / len(k)) + 1) / 2 * most**2
    basis = y[:, None] ** np.arange(terms)[None, :]
    return np.linalg.lstsq(basis, fn(np.sqrt(y)), rcond=None)[0]


COS = [float(c) for c in even_series(np.cos, 8, 2.5)]
SIN = [float(c) for c in even_series(lambda x: np.sin(x) / x, 8, 2.5)]


def cos_sin(x):
    y = x * x
    c, s = COS[-1], SIN[-1]
    for a, b in zip(COS[-2::-1], SIN[-2::-1]):
        c = c * y + a
        s = s * y + b
    return c, s * x


def turn_matrix(cos, sin, bits, left):
    size = 128 if bits is None else bits
    shape = (size, size)
    i = lax.broadcasted_iota(jnp.int32, shape, 1 if left else 0)
    j = lax.broadcasted_iota(jnp.int32, shape, 0 if left else 1)
    total = None
    for bit in range(len(cos)):
        a, b = (i >> bit) & 1, (j >> bit) & 1
        one = jnp.where(a == b, cos[bit], jnp.where(a > b, -sin[bit], sin[bit]))
        total = one if total is None else total * one
    return total


def butterflies(tiles, cos, sin):
    tiles = list(tiles)
    step = 1
    while step < len(tiles):
        for i in range(len(tiles)):
            if not i & step:
                u, v = tiles[i], tiles[i + step]
                tiles[i], tiles[i + step] = cos * u - sin * v, cos * v + sin * u
        step *= 2
    return tiles


def dot(a, b):
    return jnp.dot(a, b, precision=lax.Precision.HIGHEST, preferred_element_type=F32)


def kernel(
    n, wave, table, phase, mix, out, marg,
    s1, r1, s2, r2, m2, s3, r3, s4, r4, sq, rq, rt, rt2, cs, sn, mats,
    ssem, rsem, tssem, trsem,
):
    h, l = lax.axis_index("high"), lax.axis_index("low")
    half = n // 2

    def high(p):
        return (p, l)

    def low(q):
        return (h, q)

    barrier = pltpu.get_barrier_semaphore()

    def greet(d, _):
        pl.semaphore_signal(barrier, inc=1, device_id=high(lax.rem(h + d, n)), device_id_type=MESH)
        pl.semaphore_signal(barrier, inc=1, device_id=low(lax.rem(l + d, n)), device_id_type=MESH)
        return 0

    lax.fori_loop(1, n, greet, 0)

    def send_all(me, to, src_of, dst, send_sem, recv_sem):
        def one(p):
            pltpu.make_async_remote_copy(
                src_ref=src_of(p), dst_ref=dst, send_sem=send_sem, recv_sem=recv_sem,
                device_id=to(p), device_id_type=MESH,
            ).start()

        def both(d, _):
            one(lax.rem(me + d, n))
            one(lax.rem(me + n - d, n))
            return 0

        lax.fori_loop(1, half, both, 0)
        one(lax.rem(me + half, n))

    def waiter(ref, send_sem, recv_sem):
        return pltpu.make_async_remote_copy(
            src_ref=ref, dst_ref=ref, send_sem=send_sem, recv_sem=recv_sem,
            device_id=high(lax.rem(h + 1, n)), device_id_type=MESH,
        )

    mc, ms = cos_sin(mix[...])

    def of(layer, group):
        return mc[layer : layer + 1, group : group + 1], ms[layer : layer + 1, group : group + 1]

    row_bits = (n * SUB).bit_length() - 1
    lane_bits = LANES.bit_length() - 1
    c0, s0 = of(0, 1)
    mats[0, : n * SUB, : n * SUB] = turn_matrix([c0] * row_bits, [s0] * row_bits, n * SUB, True)
    c0, s0 = of(0, 0)
    mats[1] = turn_matrix([c0] * lane_bits, [s0] * lane_bits, LANES, False)
    c1, s1_ = of(1, 1)
    c2, s2_ = of(1, 2)
    mats[2, : n * SUB, : n * SUB] = turn_matrix(
        [c1] * 3 + [c2] * (row_bits - 3), [s1_] * 3 + [s2_] * (row_bits - 3), n * SUB, True
    )
    c1, s1_ = of(1, 0)
    mats[3] = turn_matrix([c1] * lane_bits, [s1_] * lane_bits, LANES, False)

    def wide(pair):
        return tuple(jnp.broadcast_to(x, (SUB, LANES)) for x in pair)

    pl.semaphore_wait(barrier, 2 * (n - 1))

    send_all(h, high, lambda p: table.at[:, p], rt.at[:, h], tssem.at[0], trsem.at[0])
    rt[:, pl.ds(h, 1)] = table[:, pl.ds(h, 1)]

    def first(t, _):
        angle = phase[0:1, :]
        co, si = cos_sin(table[t] * angle[None])
        re, im = wave[0, t], wave[1, t]
        for c, x in enumerate((re * co + im * si, im * co - re * si)):
            x = x.reshape(n * SUB, LANES)
            x = dot(dot(mats[0, : n * SUB, : n * SUB], x), mats[1])
            s1[t, :, c] = x.reshape(n, SUB, LANES)
        send_all(h, high, lambda p: s1.at[t, p], r1.at[t, h], ssem.at[0, t], rsem.at[0, t])
        r1[t, pl.ds(h, 1)] = s1[t, pl.ds(h, 1)]
        return 0

    lax.fori_loop(0, T, first, 0)

    waiter(rt.at[:, pl.ds(0, n - 1)], tssem.at[0], trsem.at[0]).wait_recv()
    send_all(l, low, lambda q: rt.at[:, q], rt2.at[:, l], tssem.at[1], trsem.at[1])
    rt2[:, pl.ds(l, 1)] = rt[:, pl.ds(l, 1)]

    hc, hs = wide(of(0, 2))

    def second(t, _):
        waiter(r1.at[t, pl.ds(0, n - 1)], ssem.at[0, t], rsem.at[0, t]).wait_recv()
        for c in range(2):
            tiles = butterflies([r1[t, i, c] for i in range(n)], hc, hs)
            for i in range(n):
                s2[t, i, c] = tiles[i]
        send_all(l, low, lambda q: s2.at[t, q], r2.at[t, l], ssem.at[1, t], rsem.at[1, t])
        r2[t, pl.ds(l, 1)] = s2[t, pl.ds(l, 1)]
        return 0

    lax.fori_loop(0, T, second, 0)

    waiter(rt2.at[:, pl.ds(0, n - 1)], tssem.at[1], trsem.at[1]).wait_recv()

    def factors(t, _):
        angle = phase[1:2, :]
        cs[t], sn[t] = cos_sin(rt2[t] * angle[None])
        return 0

    lax.fori_loop(0, T, factors, 0)

    lc, ls = wide(of(0, 3))

    def third(t, _):
        waiter(r2.at[t, pl.ds(0, n - 1)], ssem.at[1, t], rsem.at[1, t]).wait_recv()
        for c in range(2):
            tiles = butterflies([r2[t, i, c] for i in range(n)], lc, ls)
            for i in range(n):
                m2[t, i, c] = tiles[i]
        return 0

    lax.fori_loop(0, T, third, 0)

    tc2, ts2 = wide(of(1, 2))

    def middle(i, _):
        re = butterflies([m2[t, i, 0] for t in range(T)], hc, hs)
        im = butterflies([m2[t, i, 1] for t in range(T)], hc, hs)
        turned = ([], [])
        for t in range(T):
            co, si = cs[t, i], sn[t, i]
            turned[0].append(re[t] * co + im[t] * si)
            turned[1].append(im[t] * co - re[t] * si)
        for c in range(2):
            for t, x in enumerate(butterflies(turned[c], tc2, ts2)):
                m2[t, i, c] = x
        return 0

    lax.fori_loop(0, n, middle, 0)

    lc2, ls2 = wide(of(1, 3))

    def fourth(t, _):
        for c in range(2):
            tiles = butterflies([m2[t, i, c] for i in range(n)], lc2, ls2)
            for i in range(n):
                s3[t, i, c] = tiles[i]
        send_all(l, low, lambda q: s3.at[t, q], r3.at[t, l], ssem.at[2, t], rsem.at[2, t])
        r3[t, pl.ds(l, 1)] = s3[t, pl.ds(l, 1)]
        return 0

    lax.fori_loop(0, T, fourth, 0)

    def fifth(t, _):
        waiter(r3.at[t, pl.ds(0, n - 1)], ssem.at[2, t], rsem.at[2, t]).wait_recv()
        for c in range(2):
            x = r3[t, :, c].reshape(n * SUB, LANES)
            x = dot(dot(mats[2, : n * SUB, : n * SUB], x), mats[3])
            s4[t, :, c] = x.reshape(n, SUB, LANES)
        send_all(h, high, lambda p: s4.at[t, p], r4.at[t, h], ssem.at[3, t], rsem.at[3, t])
        r4[t, pl.ds(h, 1)] = s4[t, pl.ds(h, 1)]
        return 0

    lax.fori_loop(0, T, fifth, 0)

    rc, rs = wide(of(1, 1))

    def last(t, _):
        waiter(r4.at[t, pl.ds(0, n - 1)], ssem.at[3, t], rsem.at[3, t]).wait_recv()
        re = butterflies([r4[t, i, 0] for i in range(n)], rc, rs)
        im = butterflies([r4[t, i, 1] for i in range(n)], rc, rs)
        for i in range(n):
            out[0, t, i] = re[i]
            out[1, t, i] = im[i]
            sq[t, i] = re[i] * re[i] + im[i] * im[i]
        send_all(h, high, lambda p: sq.at[t, p], rq.at[t, h], ssem.at[4, t], rsem.at[4, t])
        rq[t, pl.ds(h, 1)] = sq[t, pl.ds(h, 1)]
        return 0

    lax.fori_loop(0, T, last, 0)

    def mean(t, _):
        waiter(rq.at[t, pl.ds(0, n - 1)], ssem.at[4, t], rsem.at[4, t]).wait_recv()
        total = rq[t, 0]
        for i in range(1, n):
            total = total + rq[t, i]
        marg[t] = total * (1.0 / n)
        return 0

    lax.fori_loop(0, T, mean, 0)

    def drain(t, _):
        for k, ref in enumerate((s1, s2, s3, s4, sq)):
            waiter(ref.at[t, pl.ds(0, n - 1)], ssem.at[k, t], rsem.at[k, t]).wait_send()
        return 0

    lax.fori_loop(0, T, drain, 0)
    waiter(rt.at[:, pl.ds(0, n - 1)], tssem.at[0], trsem.at[0]).wait_send()
    waiter(rt.at[:, pl.ds(0, n - 1)], tssem.at[1], trsem.at[1]).wait_send()


def on_device(n, wave_parts, level_table, phase_angles, mix_angles):
    wave = wave_parts.reshape(2, T, n, SUB, LANES)
    table = level_table.reshape(T, n, SUB, LANES)
    vmem = pl.BlockSpec(memory_space=pltpu.VMEM)
    state = pltpu.VMEM((T, n, 2, SUB, LANES), F32)
    half = pltpu.VMEM((T, n, SUB, LANES), F32)
    out, marg = pl.pallas_call(
        functools.partial(kernel, n),
        name="register",
        out_shape=(
            jax.ShapeDtypeStruct((2, T, n, SUB, LANES), F32),
            jax.ShapeDtypeStruct((T, SUB, LANES), F32),
        ),
        in_specs=[vmem] * 4,
        out_specs=(vmem, vmem),
        scratch_shapes=[state] * 9
        + [half] * 6
        + [
            pltpu.VMEM((4, LANES, LANES), F32),
            pltpu.SemaphoreType.DMA((5, T)),
            pltpu.SemaphoreType.DMA((5, T)),
            pltpu.SemaphoreType.DMA((2,)),
            pltpu.SemaphoreType.DMA((2,)),
        ],
        compiler_params=pltpu.CompilerParams(
            collective_id=0, has_side_effects=True, vmem_limit_bytes=24 * 1024 * 1024
        ),
    )(wave, table, phase_angles, mix_angles)
    return out.reshape(wave_parts.shape), marg


def solution(mesh):
    n = mesh.shape["high"]
    in_specs = (P(None, ("high", "low"), None, None), P(("high", "low"), None, None), P(), P())
    out_specs = (P(None, ("high", "low"), None, None), P("low", "high", None))
    return jax.shard_map(
        functools.partial(on_device, n), mesh=mesh, in_specs=in_specs, out_specs=out_specs, check_vma=False
    )
```

```python
import functools

import jax
import jax.numpy as jnp
import numpy as np
from jax import lax
from jax.experimental import pallas as pl
from jax.experimental.pallas import tpu as pltpu
from jax.sharding import PartitionSpec as P

MESH = pl.DeviceIdType.MESH
T = 4
SUB, LANES = 8, 128
F32 = jnp.float32


def even_series(fn, terms, most):
    k = np.arange(4 * terms)
    y = (np.cos((k + 0.5) * np.pi / len(k)) + 1) / 2 * most**2
    basis = y[:, None] ** np.arange(terms)[None, :]
    return np.linalg.lstsq(basis, fn(np.sqrt(y)), rcond=None)[0]


COS = [float(c) for c in even_series(np.cos, 8, 2.5)]
SIN = [float(c) for c in even_series(lambda x: np.sin(x) / x, 8, 2.5)]


def cos_sin(x):
    y = x * x
    c, s = COS[-1], SIN[-1]
    for a, b in zip(COS[-2::-1], SIN[-2::-1]):
        c = c * y + a
        s = s * y + b
    return c, s * x


def turn_matrix(cos, sin, bits, left):
    size = 128 if bits is None else bits
    shape = (size, size)
    i = lax.broadcasted_iota(jnp.int32, shape, 1 if left else 0)
    j = lax.broadcasted_iota(jnp.int32, shape, 0 if left else 1)
    total = None
    for bit in range(len(cos)):
        a, b = (i >> bit) & 1, (j >> bit) & 1
        one = jnp.where(a == b, cos[bit], jnp.where(a > b, -sin[bit], sin[bit]))
        total = one if total is None else total * one
    return total


def butterflies(tiles, cos, sin):
    tiles = list(tiles)
    step = 1
    while step < len(tiles):
        for i in range(len(tiles)):
            if not i & step:
                u, v = tiles[i], tiles[i + step]
                tiles[i], tiles[i + step] = cos * u - sin * v, cos * v + sin * u
        step *= 2
    return tiles


def dot(a, b):
    return jnp.dot(a, b, precision=lax.Precision.HIGHEST, preferred_element_type=F32)


def kernel(
    n, wave_in, table_in, phase_in, mix_in, out, marg,
    wave, table, phase, mix, s1, r1, s2, r2, s3, r3, s4, r4, y, sq, rq, rt, cs, sn, mats,
    isem, ssem, rsem, tssem, trsem, qssem, qrsem,
):
    h, l = lax.axis_index("high"), lax.axis_index("low")
    rows = n * SUB

    def high(p):
        return (p, l)

    def low(q):
        return (h, q)

    loads = [
        pltpu.make_async_copy(src, dst, isem.at[k])
        for k, (src, dst) in enumerate(((mix_in, mix), (phase_in, phase), (wave_in, wave), (table_in, table)))
    ]
    for load in loads:
        load.start()

    barrier = pltpu.get_barrier_semaphore()

    def greet(device):
        pl.semaphore_signal(barrier, inc=1, device_id=device, device_id_type=MESH)

    def greet_all(d, _):
        greet(high(lax.rem(h + d, n)))
        greet(low(lax.rem(l + d, n)))
        greet((l, lax.rem(h + d, n)))
        return 0

    lax.fori_loop(1, n, greet_all, 0)

    @pl.when(h != l)
    def _():
        greet((l, h))

    def push(src, dst, device, send_sem, recv_sem):
        pltpu.make_async_remote_copy(
            src_ref=src, dst_ref=dst, send_sem=send_sem, recv_sem=recv_sem,
            device_id=device, device_id_type=MESH,
        ).start()

    def far_first(one):
        one(lax.rem(h + n // 2, n))

        def both(d, _):
            one(lax.rem(h + n // 2 + d, n))
            one(lax.rem(h + n + n // 2 - d, n))
            return 0

        lax.fori_loop(1, n // 2, both, 0)

    side = 4 if n == 16 else 2
    offsets = [(a, b) for a in range(side) for b in range(side) if a or b]
    offsets.sort(key=lambda o: -sum(min(x, side - x) for x in o))

    def send_high(t, src, dst, k):
        far_first(lambda p: push(src.at[t, p], dst.at[t, h], high(p), ssem.at[k, t], rsem.at[k, t]))
        dst[t, pl.ds(h, 1)] = src[t, pl.ds(h, 1)]

    def send_low(t, src, dst, k):
        for a, b in offsets:
            q = lax.rem(l // side + a, side) * side + lax.rem(lax.rem(l, side) + b, side)
            push(src.at[t, q], dst.at[t, l], low(q), ssem.at[k, t], rsem.at[k, t])
        dst[t, pl.ds(l, 1)] = src[t, pl.ds(l, 1)]

    def waiter(ref, send_sem, recv_sem):
        return pltpu.make_async_remote_copy(
            src_ref=ref, dst_ref=ref, send_sem=send_sem, recv_sem=recv_sem,
            device_id=high(lax.rem(h + 1, n)), device_id_type=MESH,
        )

    def arrived(t, dst, k):
        waiter(dst.at[t, pl.ds(0, n - 1)], ssem.at[k, t], rsem.at[k, t]).wait_recv()

    loads[0].wait()
    mc, ms = cos_sin(mix[...])

    def of(layer, group):
        return mc[layer : layer + 1, group : group + 1], ms[layer : layer + 1, group : group + 1]

    def wide(pair):
        return tuple(jnp.broadcast_to(x, (SUB, LANES)) for x in pair)

    def matrix(parts, size, left):
        return turn_matrix([p[0] for p in parts], [p[1] for p in parts], size, left)

    row_bits = rows.bit_length() - 1
    lane_bits = LANES.bit_length() - 1
    mats[0, :rows, :rows] = matrix([of(0, 1)] * row_bits, rows, True)
    mats[1] = matrix([of(0, 0)] * lane_bits, LANES, False)
    mats[2, :rows, :rows] = matrix([of(1, 1)] * 3 + [of(1, 2)] * (row_bits - 3), rows, True)
    mats[3] = matrix([of(1, 0)] * lane_bits, LANES, False)
    h1, l1 = wide(of(0, 2)), wide(of(0, 3))
    l2, r2w, t2 = wide(of(1, 3)), wide(of(1, 1)), wide(of(1, 2))

    def turn_sides(x, left, right):
        x = x.reshape(rows, LANES)
        return dot(dot(mats[left, :rows, :rows], x), mats[right]).reshape(n, SUB, LANES)

    for load in loads[1:]:
        load.wait()

    def first(i, _):
        parts = ([], [])
        for t in range(T):
            co, si = cos_sin(table[t, i] * phase[0:1, :])
            re, im = wave[0, t, i], wave[1, t, i]
            parts[0].append(re * co + im * si)
            parts[1].append(im * co - re * si)
        for c in range(2):
            for t, x in enumerate(butterflies(parts[c], *h1)):
                s1[t, i, c] = x
        return 0

    lax.fori_loop(0, n, first, 0)

    def rows_lanes(t):
        for c in range(2):
            s1[t, :, c] = turn_sides(s1[t, :, c], 0, 1)

    def send_table(t):
        def one(p):
            push(table.at[t, p], rt.at[t, l], (p, h), tssem.at[t], trsem.at[t])

        far_first(one)

        @pl.when(h != l)
        def _():
            one(h)

        @pl.when(h == l)
        def _():
            rt[t, pl.ds(l, 1)] = table[t, pl.ds(h, 1)]

    def turn_high(t):
        arrived(t, r1, 0)
        for c in range(2):
            tiles = butterflies([r1[t, i, c] for i in range(n)], *h1)
            for i in range(n):
                s2[t, i, c] = tiles[i]
        send_low(t, s2, r2, 1)

    def table_done(t, sent):
        @pl.when(h != l)
        def _():
            w = waiter(rt.at[t], tssem.at[t], trsem.at[t])
            w.wait_send() if sent else w.wait_recv()

        @pl.when(h == l)
        def _():
            w = waiter(rt.at[t, pl.ds(0, n - 1)], tssem.at[t], trsem.at[t])
            w.wait_send() if sent else w.wait_recv()

    def middle(t):
        table_done(t, False)

        def factors(i, _):
            co, si = cos_sin(rt[t, i] * phase[1:2, :])
            cs[t, i], sn[t, i] = co, si
            return 0

        lax.fori_loop(0, n, factors, 0)
        arrived(t, r2, 1)
        re = butterflies([r2[t, i, 0] for i in range(n)], *l1)
        im = butterflies([r2[t, i, 1] for i in range(n)], *l1)
        turned = ([], [])
        for i in range(n):
            co, si = cs[t, i], sn[t, i]
            turned[0].append(re[i] * co + im[i] * si)
            turned[1].append(im[i] * co - re[i] * si)
        for c in range(2):
            for i, x in enumerate(butterflies(turned[c], *l2)):
                s3[t, i, c] = x
        send_low(t, s3, r3, 2)

    def turn_back(t):
        arrived(t, r3, 2)
        for c in range(2):
            s4[t, :, c] = turn_sides(r3[t, :, c], 2, 3)
        send_high(t, s4, r4, 3)

    def turn_rows(t):
        arrived(t, r4, 3)
        for c in range(2):
            tiles = butterflies([r4[t, i, c] for i in range(n)], *r2w)
            for i in range(n):
                y[t, i, c] = tiles[i]

    rows_lanes(0)
    total = 3 * (n - 1)
    pl.semaphore_wait(barrier, jnp.where(h == l, total, total + 1))
    send_high(0, s1, r1, 0)
    for t in range(1, T):
        rows_lanes(t)
        send_high(t, s1, r1, 0)
        if t >= 1:
            send_table(t - 1)
    send_table(T - 1)

    turn_high(0)
    turn_high(1)
    middle(0)
    turn_high(2)
    middle(1)
    turn_back(0)
    turn_high(3)
    middle(2)
    turn_back(1)
    middle(3)
    turn_back(2)
    turn_back(3)
    for t in range(T):
        turn_rows(t)

    def finish(p):
        re = butterflies([y[t, p, 0] for t in range(T)], *t2)
        im = butterflies([y[t, p, 1] for t in range(T)], *t2)
        for t in range(T):
            out[0, t, pl.ds(p, 1)] = re[t][None]
            out[1, t, pl.ds(p, 1)] = im[t][None]
            sq[p, t] = re[t] * re[t] + im[t] * im[t]

    def share(p):
        finish(p)
        push(sq.at[p], rq.at[h], high(p), qssem, qrsem)

    far_first(share)
    finish(h)
    rq[pl.ds(h, 1)] = sq[pl.ds(h, 1)]
    waiter(rq.at[pl.ds(0, n - 1)], qssem, qrsem).wait_recv()
    for t in range(T):
        total = rq[0, t]
        for i in range(1, n):
            total = total + rq[i, t]
        marg[t] = total * (1.0 / n)

    for t in range(T):
        for k, ref in enumerate((s1, s2, s3, s4)):
            waiter(ref.at[t, pl.ds(0, n - 1)], ssem.at[k, t], rsem.at[k, t]).wait_send()
        table_done(t, True)
    waiter(sq.at[pl.ds(0, n - 1)], qssem, qrsem).wait_send()


def on_device(n, wave_parts, level_table, phase_angles, mix_angles):
    wave = wave_parts.reshape(2, T, n, SUB, LANES)
    table = level_table.reshape(T, n, SUB, LANES)
    vmem, hbm = pl.BlockSpec(memory_space=pltpu.VMEM), pl.BlockSpec(memory_space=pltpu.HBM)
    state = pltpu.VMEM((T, n, 2, SUB, LANES), F32)
    half = pltpu.VMEM((T, n, SUB, LANES), F32)
    share = pltpu.VMEM((n, T, SUB, LANES), F32)
    dma = pltpu.SemaphoreType.DMA
    out, marg = pl.pallas_call(
        functools.partial(kernel, n),
        name="register",
        out_shape=(
            jax.ShapeDtypeStruct((2, T, n, SUB, LANES), F32),
            jax.ShapeDtypeStruct((T, SUB, LANES), F32),
        ),
        in_specs=[hbm] * 4,
        out_specs=(vmem, vmem),
        scratch_shapes=[
            pltpu.VMEM(wave.shape, F32),
            half,
            pltpu.VMEM(phase_angles.shape, F32),
            pltpu.VMEM(mix_angles.shape, F32),
        ]
        + [state] * 9
        + [share] * 2
        + [half] * 3
        + [pltpu.VMEM((4, LANES, LANES), F32)]
        + [dma((4,)), dma((4, T)), dma((4, T)), dma((T,)), dma((T,)), dma, dma],
        compiler_params=pltpu.CompilerParams(
            collective_id=0, has_side_effects=True, vmem_limit_bytes=24 * 1024 * 1024
        ),
    )(*(pltpu.with_memory_space_constraint(x, pltpu.HBM) for x in (wave, table, phase_angles, mix_angles)))
    return out.reshape(wave_parts.shape), marg


def solution(mesh):
    n = mesh.shape["high"]
    in_specs = (P(None, ("high", "low"), None, None), P(("high", "low"), None, None), P(), P())
    out_specs = (P(None, ("high", "low"), None, None), P("low", "high", None))
    return jax.shard_map(
        functools.partial(on_device, n), mesh=mesh, in_specs=in_specs, out_specs=out_specs, check_vma=False
    )
```

```python
import functools

import jax
import jax.numpy as jnp
import numpy as np
from jax import lax
from jax.experimental import pallas as pl
from jax.experimental.pallas import tpu as pltpu
from jax.sharding import PartitionSpec as P

MESH = pl.DeviceIdType.MESH
T = 4
SUB, LANES = 8, 128
F32 = jnp.float32


def even_series(fn, terms, most):
    k = np.arange(4 * terms)
    y = (np.cos((k + 0.5) * np.pi / len(k)) + 1) / 2 * most**2
    basis = y[:, None] ** np.arange(terms)[None, :]
    return np.linalg.lstsq(basis, fn(np.sqrt(y)), rcond=None)[0]


COS = [float(c) for c in even_series(np.cos, 8, 2.5)]
SIN = [float(c) for c in even_series(lambda x: np.sin(x) / x, 8, 2.5)]


def cos_sin(x):
    y = x * x
    c, s = COS[-1], SIN[-1]
    for a, b in zip(COS[-2::-1], SIN[-2::-1]):
        c = c * y + a
        s = s * y + b
    return c, s * x


def turn_matrix(cos, sin, bits, left):
    size = 128 if bits is None else bits
    shape = (size, size)
    i = lax.broadcasted_iota(jnp.int32, shape, 1 if left else 0)
    j = lax.broadcasted_iota(jnp.int32, shape, 0 if left else 1)
    total = None
    for bit in range(len(cos)):
        a, b = (i >> bit) & 1, (j >> bit) & 1
        one = jnp.where(a == b, cos[bit], jnp.where(a > b, -sin[bit], sin[bit]))
        total = one if total is None else total * one
    return total


def butterflies(tiles, cos, sin):
    tiles = list(tiles)
    step = 1
    while step < len(tiles):
        for i in range(len(tiles)):
            if not i & step:
                u, v = tiles[i], tiles[i + step]
                tiles[i], tiles[i + step] = cos * u - sin * v, cos * v + sin * u
        step *= 2
    return tiles


def split(x):
    top = x.astype(jnp.bfloat16)
    return top, (x - top.astype(F32)).astype(jnp.bfloat16)


def dot(a, b):
    return sum(jnp.dot(x, y, preferred_element_type=F32) for x, y in ((a[0], b[0]), (a[0], b[1]), (a[1], b[0])))


def kernel(
    n, wave_in, table_in, phase_in, mix_in, out, marg,
    wave, table, phase, mix, s1, r1, s2, r2, s3, r3, s4, r4, y, sq, pre, tot, rq, rt, cs, sn, mats,
    ready, isem, ssem, rsem, tssem, trsem, pssem, prsem, qssem, qrsem,
):
    h, l = lax.axis_index("high"), lax.axis_index("low")
    rows = n * SUB

    def high(p):
        return (p, l)

    def low(q):
        return (h, q)

    loads = [
        pltpu.make_async_copy(src, dst, isem.at[k])
        for k, (src, dst) in enumerate(((mix_in, mix), (phase_in, phase), (wave_in, wave), (table_in, table)))
    ]
    for load in loads:
        load.start()

    barrier = pltpu.get_barrier_semaphore()

    def greet(device):
        pl.semaphore_signal(barrier, inc=1, device_id=device, device_id_type=MESH)

    def greet_all(d, _):
        greet(high(lax.rem(h + d, n)))
        greet(low(lax.rem(l + d, n)))
        return 0

    lax.fori_loop(1, n, greet_all, 0)

    def push(src, dst, device, send_sem, recv_sem):
        pltpu.make_async_remote_copy(
            src_ref=src, dst_ref=dst, send_sem=send_sem, recv_sem=recv_sem,
            device_id=device, device_id_type=MESH,
        ).start()

    def far_first(one):
        one(lax.rem(h + n // 2, n))

        def both(d, _):
            one(lax.rem(h + n // 2 + d, n))
            one(lax.rem(h + n + n // 2 - d, n))
            return 0

        lax.fori_loop(1, n // 2, both, 0)

    side = 4 if n == 16 else 2
    offsets = [(a, b) for a in range(side) for b in range(side) if a or b]
    offsets.sort(key=lambda o: -sum(min(x, side - x) for x in o))

    def send_high(t, c, src, dst, k):
        far_first(lambda p: push(src.at[t, c, p], dst.at[t, c, h], high(p), ssem.at[k, t, c], rsem.at[k, t, c]))
        dst[t, c, pl.ds(h, 1)] = src[t, c, pl.ds(h, 1)]

    def send_low(t, c, src, dst, k):
        for a, b in offsets:
            q = lax.rem(l // side + a, side) * side + lax.rem(lax.rem(l, side) + b, side)
            push(src.at[t, c, q], dst.at[t, c, l], low(q), ssem.at[k, t, c], rsem.at[k, t, c])
        dst[t, c, pl.ds(l, 1)] = src[t, c, pl.ds(l, 1)]

    def waiter(ref, send_sem, recv_sem):
        return pltpu.make_async_remote_copy(
            src_ref=ref, dst_ref=ref, send_sem=send_sem, recv_sem=recv_sem,
            device_id=high(lax.rem(h + 1, n)), device_id_type=MESH,
        )

    def arrived(t, c, dst, k):
        waiter(dst.at[t, c, pl.ds(0, n - 1)], ssem.at[k, t, c], rsem.at[k, t, c]).wait_recv()

    loads[0].wait()
    mc, ms = cos_sin(mix[...])

    def of(layer, group):
        return mc[layer : layer + 1, group : group + 1], ms[layer : layer + 1, group : group + 1]

    def wide(pair):
        return tuple(jnp.broadcast_to(x, (SUB, LANES)) for x in pair)

    def matrix(parts, size, left):
        return turn_matrix([p[0] for p in parts], [p[1] for p in parts], size, left)

    row_bits = rows.bit_length() - 1
    lane_bits = LANES.bit_length() - 1
    for k, made in enumerate(
        (
            matrix([of(0, 1)] * row_bits, rows, True),
            matrix([of(0, 0)] * lane_bits, LANES, False),
            matrix([of(1, 1)] * 3 + [of(1, 2)] * (row_bits - 3), rows, True),
            matrix([of(1, 0)] * lane_bits, LANES, False),
        )
    ):
        size = made.shape[0]
        mats[k, 0, :size, :size], mats[k, 1, :size, :size] = split(made)
    h1, l1 = wide(of(0, 2)), wide(of(0, 3))
    l2, r2w, t2 = wide(of(1, 3)), wide(of(1, 1)), wide(of(1, 2))

    def turn_sides(x, left, right):
        x = dot((mats[left, 0, :rows, :rows], mats[left, 1, :rows, :rows]), split(x.reshape(rows, LANES)))
        return dot(split(x), (mats[right, 0], mats[right, 1])).reshape(n, SUB, LANES)

    for load in loads[1:]:
        load.wait()

    def first(i, _):
        parts = ([], [])
        for t in range(T):
            co, si = cos_sin(table[t, i] * phase[0:1, :])
            re, im = wave[0, t, i], wave[1, t, i]
            parts[0].append(re * co + im * si)
            parts[1].append(im * co - re * si)
        for c in range(2):
            for t, x in enumerate(butterflies(parts[c], *h1)):
                s1[t, c, i] = x
        return 0

    lax.fori_loop(0, n, first, 0)

    def rows_lanes(t):
        for c in range(2):
            s1[t, c] = turn_sides(s1[t, c], 0, 1)

    def send_table(t):
        def one(p):
            push(table.at[t, p], rt.at[t, l], (p, h), tssem.at[t], trsem.at[t])

        far_first(one)

        @pl.when(h != l)
        def _():
            one(h)

        @pl.when(h == l)
        def _():
            rt[t, pl.ds(l, 1)] = table[t, pl.ds(h, 1)]

    def turn_high(t):
        for c in range(2):
            arrived(t, c, r1, 0)
            tiles = butterflies([r1[t, c, i] for i in range(n)], *h1)
            for i in range(n):
                s2[t, c, i] = tiles[i]
            send_low(t, c, s2, r2, 1)

    def table_done(t, sent):
        @pl.when(h != l)
        def _():
            w = waiter(rt.at[t], tssem.at[t], trsem.at[t])
            w.wait_send() if sent else w.wait_recv()

        @pl.when(h == l)
        def _():
            w = waiter(rt.at[t, pl.ds(0, n - 1)], tssem.at[t], trsem.at[t])
            w.wait_send() if sent else w.wait_recv()

    def middle(t):
        table_done(t, False)

        def factors(i, _):
            co, si = cos_sin(rt[t, i] * phase[1:2, :])
            cs[t, i], sn[t, i] = co, si
            return 0

        lax.fori_loop(0, n, factors, 0)
        arrived(t, 0, r2, 1)
        re = butterflies([r2[t, 0, i] for i in range(n)], *l1)
        arrived(t, 1, r2, 1)
        im = butterflies([r2[t, 1, i] for i in range(n)], *l1)
        turned = ([], [])
        for i in range(n):
            co, si = cs[t, i], sn[t, i]
            turned[0].append(re[i] * co + im[i] * si)
            turned[1].append(im[i] * co - re[i] * si)
        for c in range(2):
            for i, x in enumerate(butterflies(turned[c], *l2)):
                s3[t, c, i] = x
            send_low(t, c, s3, r3, 2)

    def turn_back(t):
        for c in range(2):
            arrived(t, c, r3, 2)
            s4[t, c] = turn_sides(r3[t, c], 2, 3)
            send_high(t, c, s4, r4, 3)

    def turn_rows(t):
        for c in range(2):
            arrived(t, c, r4, 3)
            tiles = butterflies([r4[t, c, i] for i in range(n)], *r2w)
            for i in range(n):
                y[t, c, i] = tiles[i]

    rows_lanes(0)
    pl.semaphore_wait(barrier, 2 * (n - 1))
    send_high(0, 0, s1, r1, 0)
    send_high(0, 1, s1, r1, 0)

    def tell(d, _):
        pl.semaphore_signal(ready, inc=1, device_id=low(lax.rem(l + d, n)), device_id_type=MESH)
        return 0

    lax.fori_loop(1, n, tell, 0)
    for t in range(1, T):
        rows_lanes(t)
        send_high(t, 0, s1, r1, 0)
        send_high(t, 1, s1, r1, 0)
        if t == 1:
            pl.semaphore_wait(ready, n - 1)
        send_table(t - 1)
    send_table(T - 1)

    turn_high(0)
    turn_high(1)
    middle(0)
    turn_high(2)
    middle(1)
    turn_back(0)
    turn_high(3)
    middle(2)
    turn_back(1)
    middle(3)
    turn_back(2)
    turn_back(3)
    for t in range(T):
        turn_rows(t)

    def finish(p):
        re = butterflies([y[t, 0, p] for t in range(T)], *t2)
        im = butterflies([y[t, 1, p] for t in range(T)], *t2)
        for t in range(T):
            out[0, t, pl.ds(p, 1)] = re[t][None]
            out[1, t, pl.ds(p, 1)] = im[t][None]
            sq[p, t] = re[t] * re[t] + im[t] * im[t]

    chips = n // 2
    z, core = h // 2, lax.rem(h, 2)

    def chips_far_first(one):
        one(lax.rem(z + chips // 2, chips))

        def both(d, _):
            one(lax.rem(z + chips // 2 + d, chips))
            one(lax.rem(z + chips + chips // 2 - d, chips))
            return 0

        lax.fori_loop(1, chips // 2, both, 0)

    def to_sibling(v):
        p = 2 * v + 1 - core
        finish(p)
        push(sq.at[p], pre.at[v], high(2 * z + 1 - core), pssem.at[v], prsem.at[v])
        finish(2 * v + core)

    def both_cores(v):
        waiter(pre.at[v], pssem.at[v], prsem.at[v]).wait_recv()
        tot[v] = sq[2 * v + core] + pre[v]

    def to_chip(v):
        both_cores(v)
        push(tot.at[v], rq.at[z], high(2 * v + core), qssem, qrsem)

    chips_far_first(to_sibling)
    to_sibling(z)
    chips_far_first(to_chip)
    both_cores(z)
    rq[pl.ds(z, 1)] = tot[pl.ds(z, 1)]
    waiter(rq.at[pl.ds(0, chips - 1)], qssem, qrsem).wait_recv()
    for t in range(T):
        total = rq[0, t]
        for i in range(1, chips):
            total = total + rq[i, t]
        marg[t] = total * (1.0 / n)

    for t in range(T):
        for k, ref in enumerate((s1, s2, s3, s4)):
            for c in range(2):
                waiter(ref.at[t, c, pl.ds(0, n - 1)], ssem.at[k, t, c], rsem.at[k, t, c]).wait_send()
        table_done(t, True)
    for v in range(chips):
        waiter(pre.at[v], pssem.at[v], prsem.at[v]).wait_send()
    waiter(tot.at[pl.ds(0, chips - 1)], qssem, qrsem).wait_send()


def put_out(state, marg, state_out, marg_out, sem):
    copies = [
        pltpu.make_async_copy(src, dst, sem.at[k]) for k, (src, dst) in enumerate(((state, state_out), (marg, marg_out)))
    ]
    for copy in copies:
        copy.start()
    for copy in copies:
        copy.wait()


def on_device(n, wave_parts, level_table, phase_angles, mix_angles):
    wave = wave_parts.reshape(2, T, n, SUB, LANES)
    table = level_table.reshape(T, n, SUB, LANES)
    vmem, hbm = pl.BlockSpec(memory_space=pltpu.VMEM), pl.BlockSpec(memory_space=pltpu.HBM)
    state = pltpu.VMEM((T, 2, n, SUB, LANES), F32)
    half = pltpu.VMEM((T, n, SUB, LANES), F32)
    def share(count):
        return pltpu.VMEM((count, T, SUB, LANES), F32)

    dma = pltpu.SemaphoreType.DMA
    out, marg = pl.pallas_call(
        functools.partial(kernel, n),
        name="register",
        out_shape=(
            jax.ShapeDtypeStruct((2, T, n, SUB, LANES), F32),
            jax.ShapeDtypeStruct((T, SUB, LANES), F32),
        ),
        in_specs=[hbm] * 4,
        out_specs=(vmem, vmem),
        scratch_shapes=[
            pltpu.VMEM(wave.shape, F32),
            half,
            pltpu.VMEM(phase_angles.shape, F32),
            pltpu.VMEM(mix_angles.shape, F32),
        ]
        + [state] * 9
        + [share(n)]
        + [share(n // 2)] * 3
        + [half] * 3
        + [pltpu.VMEM((4, 2, LANES, LANES), jnp.bfloat16)]
        + [pltpu.SemaphoreType.REGULAR, dma((4,)), dma((4, T, 2)), dma((4, T, 2)), dma((T,)), dma((T,))]
        + [dma((n // 2,)), dma((n // 2,)), dma, dma],
        compiler_params=pltpu.CompilerParams(
            collective_id=0, has_side_effects=True, vmem_limit_bytes=24 * 1024 * 1024
        ),
    )(*(pltpu.with_memory_space_constraint(x, pltpu.HBM) for x in (wave, table, phase_angles, mix_angles)))
    out, marg = pl.pallas_call(
        put_out,
        name="put_out",
        out_shape=(jax.ShapeDtypeStruct(out.shape, F32), jax.ShapeDtypeStruct(marg.shape, F32)),
        in_specs=[vmem] * 2,
        out_specs=(hbm, hbm),
        scratch_shapes=[dma((2,))],
        compiler_params=pltpu.CompilerParams(vmem_limit_bytes=8 * 1024 * 1024),
    )(out, marg)
    return out.reshape(wave_parts.shape), marg


def solution(mesh):
    n = mesh.shape["high"]
    in_specs = (P(None, ("high", "low"), None, None), P(("high", "low"), None, None), P(), P())
    out_specs = (P(None, ("high", "low"), None, None), P("low", "high", None))
    return jax.shard_map(
        functools.partial(on_device, n), mesh=mesh, in_specs=in_specs, out_specs=out_specs, check_vma=False
    )
```

```python
import functools

import jax
import jax.numpy as jnp
import numpy as np
from jax import lax
from jax.experimental import pallas as pl
from jax.experimental.pallas import tpu as pltpu
from jax.sharding import PartitionSpec as P

MESH = pl.DeviceIdType.MESH
T = 4
SUB, LANES = 8, 128
F32 = jnp.float32


def even_series(fn, terms, most):
    k = np.arange(4 * terms)
    y = (np.cos((k + 0.5) * np.pi / len(k)) + 1) / 2 * most**2
    basis = y[:, None] ** np.arange(terms)[None, :]
    return np.linalg.lstsq(basis, fn(np.sqrt(y)), rcond=None)[0]


COS = [float(c) for c in even_series(np.cos, 8, 2.5)]
SIN = [float(c) for c in even_series(lambda x: np.sin(x) / x, 8, 2.5)]


def cos_sin(x):
    y = x * x
    c, s = COS[-1], SIN[-1]
    for a, b in zip(COS[-2::-1], SIN[-2::-1]):
        c = c * y + a
        s = s * y + b
    return c, s * x


def turn_matrix(cos, sin, bits, left):
    size = 128 if bits is None else bits
    shape = (size, size)
    i = lax.broadcasted_iota(jnp.int32, shape, 1 if left else 0)
    j = lax.broadcasted_iota(jnp.int32, shape, 0 if left else 1)
    total = None
    for bit in range(len(cos)):
        a, b = (i >> bit) & 1, (j >> bit) & 1
        one = jnp.where(a == b, cos[bit], jnp.where(a > b, -sin[bit], sin[bit]))
        total = one if total is None else total * one
    return total


def butterflies(tiles, cos, sin):
    tiles = list(tiles)
    step = 1
    while step < len(tiles):
        for i in range(len(tiles)):
            if not i & step:
                u, v = tiles[i], tiles[i + step]
                tiles[i], tiles[i + step] = cos * u - sin * v, cos * v + sin * u
        step *= 2
    return tiles


def split(x):
    top = x.astype(jnp.bfloat16)
    return top, (x - top.astype(F32)).astype(jnp.bfloat16)


def dot(a, b):
    return sum(jnp.dot(x, y, preferred_element_type=F32) for x, y in ((a[0], b[0]), (a[0], b[1]), (a[1], b[0])))


def kernel(
    n, wave_in, table_in, phase_in, mix_in, out, marg,
    wave, table, phase, mix, s1, r1, s2, r2, s3, r3, s4, r4, y, sq, pre, tot, rq, rt, cs, sn, mats,
    ready, isem, ssem, rsem, tssem, trsem, pssem, prsem, qssem, qrsem,
):
    h, l = lax.axis_index("high"), lax.axis_index("low")
    rows = n * SUB

    def high(p):
        return (p, l)

    def low(q):
        return (h, q)

    loads = [
        pltpu.make_async_copy(src, dst, isem.at[k])
        for k, (src, dst) in enumerate(((mix_in, mix), (phase_in, phase), (wave_in, wave), (table_in, table)))
    ]
    for load in loads:
        load.start()

    barrier = pltpu.get_barrier_semaphore()

    def greet(device):
        pl.semaphore_signal(barrier, inc=1, device_id=device, device_id_type=MESH)

    def greet_all(d, _):
        greet(high(lax.rem(h + d, n)))
        greet(low(lax.rem(l + d, n)))
        return 0

    lax.fori_loop(1, n, greet_all, 0)

    def push(src, dst, device, send_sem, recv_sem):
        pltpu.make_async_remote_copy(
            src_ref=src, dst_ref=dst, send_sem=send_sem, recv_sem=recv_sem,
            device_id=device, device_id_type=MESH,
        ).start()

    def far_first(one):
        one(lax.rem(h + n // 2, n))

        def both(d, _):
            one(lax.rem(h + n // 2 + d, n))
            one(lax.rem(h + n + n // 2 - d, n))
            return 0

        lax.fori_loop(1, n // 2, both, 0)

    side = 4 if n == 16 else 2
    offsets = [(a, b) for a in range(side) for b in range(side) if a or b]
    offsets.sort(key=lambda o: -sum(min(x, side - x) for x in o))

    def send_high(t, c, src, dst, k):
        far_first(lambda p: push(src.at[t, c, p], dst.at[t, c, h], high(p), ssem.at[k, t, c], rsem.at[k, t, c]))
        dst[t, c, pl.ds(h, 1)] = src[t, c, pl.ds(h, 1)]

    def send_low(t, c, src, dst, k):
        for a, b in offsets:
            q = lax.rem(l // side + a, side) * side + lax.rem(lax.rem(l, side) + b, side)
            push(src.at[t, c, q], dst.at[t, c, l], low(q), ssem.at[k, t, c], rsem.at[k, t, c])
        dst[t, c, pl.ds(l, 1)] = src[t, c, pl.ds(l, 1)]

    def waiter(ref, send_sem, recv_sem):
        return pltpu.make_async_remote_copy(
            src_ref=ref, dst_ref=ref, send_sem=send_sem, recv_sem=recv_sem,
            device_id=high(lax.rem(h + 1, n)), device_id_type=MESH,
        )

    def arrived(t, c, dst, k):
        waiter(dst.at[t, c, pl.ds(0, n - 1)], ssem.at[k, t, c], rsem.at[k, t, c]).wait_recv()

    loads[0].wait()
    mc, ms = cos_sin(mix[...])

    def of(layer, group):
        return mc[layer : layer + 1, group : group + 1], ms[layer : layer + 1, group : group + 1]

    def wide(pair):
        return tuple(jnp.broadcast_to(x, (SUB, LANES)) for x in pair)

    def matrix(parts, size, left):
        return turn_matrix([p[0] for p in parts], [p[1] for p in parts], size, left)

    row_bits = rows.bit_length() - 1
    lane_bits = LANES.bit_length() - 1
    for k, made in enumerate(
        (
            matrix([of(0, 1)] * row_bits, rows, True),
            matrix([of(0, 0)] * lane_bits, LANES, False),
            matrix([of(1, 1)] * 3 + [of(1, 2)] * (row_bits - 3), rows, True),
            matrix([of(1, 0)] * lane_bits, LANES, False),
        )
    ):
        size = made.shape[0]
        mats[k, 0, :size, :size], mats[k, 1, :size, :size] = split(made)
    h1, l1 = wide(of(0, 2)), wide(of(0, 3))
    l2, r2w, t2 = wide(of(1, 3)), wide(of(1, 1)), wide(of(1, 2))

    def turn_sides(x, left, right):
        x = dot((mats[left, 0, :rows, :rows], mats[left, 1, :rows, :rows]), split(x.reshape(rows, LANES)))
        return dot(split(x), (mats[right, 0], mats[right, 1])).reshape(n, SUB, LANES)

    for load in loads[1:]:
        load.wait()

    def first(i, _):
        parts = ([], [])
        for t in range(T):
            co, si = cos_sin(table[t, i] * phase[0:1, :])
            re, im = wave[0, t, i], wave[1, t, i]
            parts[0].append(re * co + im * si)
            parts[1].append(im * co - re * si)
        for c in range(2):
            for t, x in enumerate(butterflies(parts[c], *h1)):
                s1[t, c, i] = x
        return 0

    lax.fori_loop(0, n, first, 0)

    def rows_lanes(t):
        for c in range(2):
            s1[t, c] = turn_sides(s1[t, c], 0, 1)

    def send_table(t):
        def one(p):
            push(table.at[t, p], rt.at[t, l], (p, h), tssem.at[t], trsem.at[t])

        far_first(one)

        @pl.when(h != l)
        def _():
            one(h)

        @pl.when(h == l)
        def _():
            rt[t, pl.ds(l, 1)] = table[t, pl.ds(h, 1)]

    def turn_high(t):
        for c in range(2):
            arrived(t, c, r1, 0)
            tiles = butterflies([r1[t, c, i] for i in range(n)], *h1)
            for i in range(n):
                s2[t, c, i] = tiles[i]
            send_low(t, c, s2, r2, 1)

    def table_done(t, sent):
        @pl.when(h != l)
        def _():
            w = waiter(rt.at[t], tssem.at[t], trsem.at[t])
            w.wait_send() if sent else w.wait_recv()

        @pl.when(h == l)
        def _():
            w = waiter(rt.at[t, pl.ds(0, n - 1)], tssem.at[t], trsem.at[t])
            w.wait_send() if sent else w.wait_recv()

    def middle(t):
        table_done(t, False)

        def factors(i, _):
            co, si = cos_sin(rt[t, i] * phase[1:2, :])
            cs[t, i], sn[t, i] = co, si
            return 0

        lax.fori_loop(0, n, factors, 0)
        arrived(t, 0, r2, 1)
        re = butterflies([r2[t, 0, i] for i in range(n)], *l1)
        arrived(t, 1, r2, 1)
        im = butterflies([r2[t, 1, i] for i in range(n)], *l1)
        turned = ([], [])
        for i in range(n):
            co, si = cs[t, i], sn[t, i]
            turned[0].append(re[i] * co + im[i] * si)
            turned[1].append(im[i] * co - re[i] * si)
        for c in range(2):
            for i, x in enumerate(butterflies(turned[c], *l2)):
                s3[t, c, i] = x
            send_low(t, c, s3, r3, 2)

    def turn_back(t):
        for c in range(2):
            arrived(t, c, r3, 2)
            s4[t, c] = turn_sides(r3[t, c], 2, 3)
            send_high(t, c, s4, r4, 3)

    def turn_rows(t):
        for c in range(2):
            arrived(t, c, r4, 3)
            tiles = butterflies([r4[t, c, i] for i in range(n)], *r2w)
            for i in range(n):
                y[t, c, i] = tiles[i]

    rows_lanes(0)
    pl.semaphore_wait(barrier, 2 * (n - 1))
    send_high(0, 0, s1, r1, 0)
    send_high(0, 1, s1, r1, 0)

    def tell(d, _):
        pl.semaphore_signal(ready, inc=1, device_id=low(lax.rem(l + d, n)), device_id_type=MESH)
        return 0

    lax.fori_loop(1, n, tell, 0)
    told = False
    for what, t in [('T', 0), ('A', 1), ('T', 1), ('A', 2), ('T', 2), ('A', 3), ('T', 3)]:
        if what == "A":
            rows_lanes(t)
            send_high(t, 0, s1, r1, 0)
            send_high(t, 1, s1, r1, 0)
        else:
            if not told:
                pl.semaphore_wait(ready, n - 1)
                told = True
            send_table(t)

    turn_high(0)
    turn_high(1)
    middle(0)
    turn_high(2)
    middle(1)
    turn_back(0)
    turn_high(3)
    middle(2)
    turn_back(1)
    middle(3)
    turn_back(2)
    turn_back(3)
    for t in range(T):
        turn_rows(t)

    def finish(p):
        re = butterflies([y[t, 0, p] for t in range(T)], *t2)
        im = butterflies([y[t, 1, p] for t in range(T)], *t2)
        for t in range(T):
            out[0, t, pl.ds(p, 1)] = re[t][None]
            out[1, t, pl.ds(p, 1)] = im[t][None]
            sq[p, t] = re[t] * re[t] + im[t] * im[t]

    chips = n // 2
    z, core = h // 2, lax.rem(h, 2)

    def chips_far_first(one):
        def each(d, _):
            one(d + (d >= z).astype(jnp.int32))
            return 0

        lax.fori_loop(0, chips - 1, each, 0)

    def to_sibling(v):
        p = 2 * v + 1 - core
        finish(p)
        push(sq.at[p], pre.at[v], high(2 * z + 1 - core), pssem.at[v], prsem.at[v])
        finish(2 * v + core)

    def both_cores(v):
        waiter(pre.at[v], pssem.at[v], prsem.at[v]).wait_recv()
        tot[v] = sq[2 * v + core] + pre[v]

    def to_chip(v):
        both_cores(v)
        push(tot.at[v], rq.at[z], high(2 * v + core), qssem, qrsem)

    chips_far_first(to_sibling)
    to_sibling(z)
    chips_far_first(to_chip)
    both_cores(z)
    rq[pl.ds(z, 1)] = tot[pl.ds(z, 1)]
    waiter(rq.at[pl.ds(0, chips - 1)], qssem, qrsem).wait_recv()
    for t in range(T):
        total = rq[0, t]
        for i in range(1, chips):
            total = total + rq[i, t]
        marg[t] = total * (1.0 / n)

    for t in range(T):
        for k, ref in enumerate((s1, s2, s3, s4)):
            for c in range(2):
                waiter(ref.at[t, c, pl.ds(0, n - 1)], ssem.at[k, t, c], rsem.at[k, t, c]).wait_send()
        table_done(t, True)
    for v in range(chips):
        waiter(pre.at[v], pssem.at[v], prsem.at[v]).wait_send()
    waiter(tot.at[pl.ds(0, chips - 1)], qssem, qrsem).wait_send()


def put_out(state, marg, state_out, marg_out, sem):
    copies = [
        pltpu.make_async_copy(src, dst, sem.at[k]) for k, (src, dst) in enumerate(((state, state_out), (marg, marg_out)))
    ]
    for copy in copies:
        copy.start()
    for copy in copies:
        copy.wait()


def on_device(n, wave_parts, level_table, phase_angles, mix_angles):
    wave = wave_parts.reshape(2, T, n, SUB, LANES)
    table = level_table.reshape(T, n, SUB, LANES)
    vmem, hbm = pl.BlockSpec(memory_space=pltpu.VMEM), pl.BlockSpec(memory_space=pltpu.HBM)
    state = pltpu.VMEM((T, 2, n, SUB, LANES), F32)
    half = pltpu.VMEM((T, n, SUB, LANES), F32)
    def share(count):
        return pltpu.VMEM((count, T, SUB, LANES), F32)

    dma = pltpu.SemaphoreType.DMA
    out, marg = pl.pallas_call(
        functools.partial(kernel, n),
        name="register",
        out_shape=(
            jax.ShapeDtypeStruct((2, T, n, SUB, LANES), F32),
            jax.ShapeDtypeStruct((T, SUB, LANES), F32),
        ),
        in_specs=[hbm] * 4,
        out_specs=(vmem, vmem),
        scratch_shapes=[
            pltpu.VMEM(wave.shape, F32),
            half,
            pltpu.VMEM(phase_angles.shape, F32),
            pltpu.VMEM(mix_angles.shape, F32),
        ]
        + [state] * 9
        + [share(n)]
        + [share(n // 2)] * 3
        + [half] * 3
        + [pltpu.VMEM((4, 2, LANES, LANES), jnp.bfloat16)]
        + [pltpu.SemaphoreType.REGULAR, dma((4,)), dma((4, T, 2)), dma((4, T, 2)), dma((T,)), dma((T,))]
        + [dma((n // 2,)), dma((n // 2,)), dma, dma],
        compiler_params=pltpu.CompilerParams(
            collective_id=0, has_side_effects=True, vmem_limit_bytes=24 * 1024 * 1024
        ),
    )(*(pltpu.with_memory_space_constraint(x, pltpu.HBM) for x in (wave, table, phase_angles, mix_angles)))
    out, marg = pl.pallas_call(
        put_out,
        name="put_out",
        out_shape=(jax.ShapeDtypeStruct(out.shape, F32), jax.ShapeDtypeStruct(marg.shape, F32)),
        in_specs=[vmem] * 2,
        out_specs=(hbm, hbm),
        scratch_shapes=[dma((2,))],
        compiler_params=pltpu.CompilerParams(vmem_limit_bytes=8 * 1024 * 1024),
    )(out, marg)
    return out.reshape(wave_parts.shape), marg


def solution(mesh):
    n = mesh.shape["high"]
    in_specs = (P(None, ("high", "low"), None, None), P(("high", "low"), None, None), P(), P())
    out_specs = (P(None, ("high", "low"), None, None), P("low", "high", None))
    return jax.shard_map(
        functools.partial(on_device, n), mesh=mesh, in_specs=in_specs, out_specs=out_specs, check_vma=False
    )
```

```python
import functools

import jax
import jax.numpy as jnp
import numpy as np
from jax import lax
from jax.experimental import pallas as pl
from jax.experimental.pallas import tpu as pltpu
from jax.sharding import PartitionSpec as P

MESH = pl.DeviceIdType.MESH
T = 4
SUB, LANES = 8, 128
F32 = jnp.float32


def even_series(fn, terms, most):
    k = np.arange(4 * terms)
    y = (np.cos((k + 0.5) * np.pi / len(k)) + 1) / 2 * most**2
    basis = y[:, None] ** np.arange(terms)[None, :]
    return np.linalg.lstsq(basis, fn(np.sqrt(y)), rcond=None)[0]


COS = [float(c) for c in even_series(np.cos, 8, 2.5)]
SIN = [float(c) for c in even_series(lambda x: np.sin(x) / x, 8, 2.5)]


def cos_sin(x):
    y = x * x
    c, s = COS[-1], SIN[-1]
    for a, b in zip(COS[-2::-1], SIN[-2::-1]):
        c = c * y + a
        s = s * y + b
    return c, s * x


def turn_matrix(cos, sin, bits, left):
    size = 128 if bits is None else bits
    shape = (size, size)
    i = lax.broadcasted_iota(jnp.int32, shape, 1 if left else 0)
    j = lax.broadcasted_iota(jnp.int32, shape, 0 if left else 1)
    total = None
    for bit in range(len(cos)):
        a, b = (i >> bit) & 1, (j >> bit) & 1
        one = jnp.where(a == b, cos[bit], jnp.where(a > b, -sin[bit], sin[bit]))
        total = one if total is None else total * one
    return total


def butterflies(tiles, cos, sin):
    tiles = list(tiles)
    step = 1
    while step < len(tiles):
        for i in range(len(tiles)):
            if not i & step:
                u, v = tiles[i], tiles[i + step]
                tiles[i], tiles[i + step] = cos * u - sin * v, cos * v + sin * u
        step *= 2
    return tiles


def split(x):
    top = x.astype(jnp.bfloat16)
    return top, (x - top.astype(F32)).astype(jnp.bfloat16)


def dot(a, b):
    return sum(jnp.dot(x, y, preferred_element_type=F32) for x, y in ((a[0], b[0]), (a[0], b[1]), (a[1], b[0])))


def kernel(
    n, wave_in, table_in, phase_in, mix_in, out, marg,
    wave, table, phase, mix, s1, r1, s2, r2, s3, r3, s4, r4, y, sq, pre, tot, rq, rt, cs, sn, mats,
    ready, isem, ssem, rsem, tssem, trsem, pssem, prsem, qssem, qrsem,
):
    h, l = lax.axis_index("high"), lax.axis_index("low")
    rows = n * SUB

    def high(p):
        return (p, l)

    def low(q):
        return (h, q)

    loads = [
        pltpu.make_async_copy(src, dst, isem.at[k])
        for k, (src, dst) in enumerate(((mix_in, mix), (phase_in, phase), (wave_in, wave), (table_in, table)))
    ]
    for load in loads:
        load.start()

    barrier = pltpu.get_barrier_semaphore()

    def greet(device):
        pl.semaphore_signal(barrier, inc=1, device_id=device, device_id_type=MESH)

    def greet_all(d, _):
        greet(high(lax.rem(h + n // 2 + d, n)))
        greet(low(lax.rem(l + n // 2 + d, n)))
        return 0

    lax.fori_loop(0, n // 2, greet_all, 0)
    lax.fori_loop(n // 2 + 1, n, greet_all, 0)

    def push(src, dst, device, send_sem, recv_sem):
        pltpu.make_async_remote_copy(
            src_ref=src, dst_ref=dst, send_sem=send_sem, recv_sem=recv_sem,
            device_id=device, device_id_type=MESH,
        ).start()

    def far_first(one):
        one(lax.rem(h + n // 2, n))

        def both(d, _):
            one(lax.rem(h + n // 2 + d, n))
            one(lax.rem(h + n + n // 2 - d, n))
            return 0

        lax.fori_loop(1, n // 2, both, 0)

    side = 4 if n == 16 else 2
    offsets = [(a, b) for a in range(side) for b in range(side) if a or b]
    offsets.sort(key=lambda o: -sum(min(x, side - x) for x in o))

    down = [lax.rem(l // side + a, side) * side for a in range(side)]
    along = [lax.rem(lax.rem(l, side) + b, side) for b in range(side)]
    peers = [down[a] + along[b] for a, b in offsets]

    def send_high(t, c, src, dst, k):
        far_first(lambda p: push(src.at[t, c, p], dst.at[t, c, h], high(p), ssem.at[k, t, c], rsem.at[k, t, c]))
        dst[t, c, pl.ds(h, 1)] = src[t, c, pl.ds(h, 1)]

    def send_low(t, c, src, dst, k):
        for q in peers:
            push(src.at[t, c, q], dst.at[t, c, l], low(q), ssem.at[k, t, c], rsem.at[k, t, c])
        dst[t, c, pl.ds(l, 1)] = src[t, c, pl.ds(l, 1)]

    def waiter(ref, send_sem, recv_sem):
        return pltpu.make_async_remote_copy(
            src_ref=ref, dst_ref=ref, send_sem=send_sem, recv_sem=recv_sem,
            device_id=high(lax.rem(h + 1, n)), device_id_type=MESH,
        )

    def arrived(t, c, dst, k):
        waiter(dst.at[t, c, pl.ds(0, n - 1)], ssem.at[k, t, c], rsem.at[k, t, c]).wait_recv()

    loads[0].wait()
    mc, ms = cos_sin(mix[...])

    def of(layer, group):
        return mc[layer : layer + 1, group : group + 1], ms[layer : layer + 1, group : group + 1]

    def wide(pair):
        return tuple(jnp.broadcast_to(x, (SUB, LANES)) for x in pair)

    def matrix(parts, size, left):
        return turn_matrix([p[0] for p in parts], [p[1] for p in parts], size, left)

    row_bits = rows.bit_length() - 1
    lane_bits = LANES.bit_length() - 1
    for k, made in enumerate(
        (
            matrix([of(0, 1)] * row_bits, rows, True),
            matrix([of(0, 0)] * lane_bits, LANES, False),
            matrix([of(1, 1)] * 3 + [of(1, 2)] * (row_bits - 3), rows, True),
            matrix([of(1, 0)] * lane_bits, LANES, False),
        )
    ):
        size = made.shape[0]
        mats[k, 0, :size, :size], mats[k, 1, :size, :size] = split(made)
    h1, l1 = wide(of(0, 2)), wide(of(0, 3))
    l2, r2w, t2 = wide(of(1, 3)), wide(of(1, 1)), wide(of(1, 2))

    def turn_sides(x, left, right):
        x = dot((mats[left, 0, :rows, :rows], mats[left, 1, :rows, :rows]), split(x.reshape(rows, LANES)))
        return dot(split(x), (mats[right, 0], mats[right, 1])).reshape(n, SUB, LANES)

    for load in loads[1:]:
        load.wait()

    def first(i, _):
        parts = ([], [])
        for t in range(T):
            co, si = cos_sin(table[t, i] * phase[0:1, :])
            re, im = wave[0, t, i], wave[1, t, i]
            parts[0].append(re * co + im * si)
            parts[1].append(im * co - re * si)
        for c in range(2):
            for t, x in enumerate(butterflies(parts[c], *h1)):
                s1[t, c, i] = x
        return 0

    lax.fori_loop(0, n, first, 0)

    def rows_lanes(t):
        for c in range(2):
            s1[t, c] = turn_sides(s1[t, c], 0, 1)

    def send_table(t):
        def one(p):
            push(table.at[t, p], rt.at[t, l], (p, h), tssem.at[t], trsem.at[t])

        far_first(one)

        @pl.when(h != l)
        def _():
            one(h)

        @pl.when(h == l)
        def _():
            rt[t, pl.ds(l, 1)] = table[t, pl.ds(h, 1)]

    def turn_high(t):
        for c in range(2):
            arrived(t, c, r1, 0)
            tiles = butterflies([r1[t, c, i] for i in range(n)], *h1)
            for i in range(n):
                s2[t, c, i] = tiles[i]
            send_low(t, c, s2, r2, 1)

    def table_done(t, sent):
        @pl.when(h != l)
        def _():
            w = waiter(rt.at[t], tssem.at[t], trsem.at[t])
            w.wait_send() if sent else w.wait_recv()

        @pl.when(h == l)
        def _():
            w = waiter(rt.at[t, pl.ds(0, n - 1)], tssem.at[t], trsem.at[t])
            w.wait_send() if sent else w.wait_recv()

    def middle(t):
        table_done(t, False)

        def factors(i, _):
            co, si = cos_sin(rt[t, i] * phase[1:2, :])
            cs[t, i], sn[t, i] = co, si
            return 0

        lax.fori_loop(0, n, factors, 0)
        arrived(t, 0, r2, 1)
        re = butterflies([r2[t, 0, i] for i in range(n)], *l1)
        arrived(t, 1, r2, 1)
        im = butterflies([r2[t, 1, i] for i in range(n)], *l1)
        turned = ([], [])
        for i in range(n):
            co, si = cs[t, i], sn[t, i]
            turned[0].append(re[i] * co + im[i] * si)
            turned[1].append(im[i] * co - re[i] * si)
        for c in range(2):
            for i, x in enumerate(butterflies(turned[c], *l2)):
                s3[t, c, i] = x
            send_low(t, c, s3, r3, 2)

    def turn_back(t):
        for c in range(2):
            arrived(t, c, r3, 2)
            s4[t, c] = turn_sides(r3[t, c], 2, 3)
            send_high(t, c, s4, r4, 3)

    def turn_rows(t):
        for c in range(2):
            arrived(t, c, r4, 3)
            tiles = butterflies([r4[t, c, i] for i in range(n)], *r2w)
            for i in range(n):
                y[t, c, i] = tiles[i]

    rows_lanes(0)
    pl.semaphore_wait(barrier, 2 * (n - 1))
    send_high(0, 0, s1, r1, 0)
    send_high(0, 1, s1, r1, 0)

    def tell(d, _):
        pl.semaphore_signal(ready, inc=1, device_id=low(lax.rem(l + d, n)), device_id_type=MESH)
        return 0

    lax.fori_loop(1, n, tell, 0)
    told = False
    for what, t in [('T', 0), ('A', 1), ('T', 1), ('A', 2), ('T', 2), ('A', 3), ('T', 3)]:
        if what == "A":
            rows_lanes(t)
            send_high(t, 0, s1, r1, 0)
            send_high(t, 1, s1, r1, 0)
        else:
            if not told:
                pl.semaphore_wait(ready, n - 1)
                told = True
            send_table(t)

    turn_high(0)
    turn_high(1)
    middle(0)
    turn_high(2)
    middle(1)
    turn_back(0)
    turn_high(3)
    middle(2)
    turn_back(1)
    middle(3)
    turn_back(2)
    turn_back(3)
    for t in range(T):
        turn_rows(t)

    def finish(p):
        re = butterflies([y[t, 0, p] for t in range(T)], *t2)
        im = butterflies([y[t, 1, p] for t in range(T)], *t2)
        for t in range(T):
            out[0, t, pl.ds(p, 1)] = re[t][None]
            out[1, t, pl.ds(p, 1)] = im[t][None]
            sq[p, t] = re[t] * re[t] + im[t] * im[t]

    chips = n // 2
    z, core = h // 2, lax.rem(h, 2)

    def chips_far_first(one):
        def each(d, _):
            one(d + (d >= z).astype(jnp.int32))
            return 0

        lax.fori_loop(0, chips - 1, each, 0)

    def to_sibling(v):
        p = 2 * v + 1 - core
        finish(p)
        push(sq.at[p], pre.at[v], high(2 * z + 1 - core), pssem.at[v], prsem.at[v])
        finish(2 * v + core)

    def both_cores(v):
        waiter(pre.at[v], pssem.at[v], prsem.at[v]).wait_recv()
        tot[v] = sq[2 * v + core] + pre[v]

    def to_chip(v):
        both_cores(v)
        push(tot.at[v], rq.at[z], high(2 * v + core), qssem, qrsem)

    chips_far_first(to_sibling)
    to_sibling(z)
    chips_far_first(to_chip)
    both_cores(z)
    rq[pl.ds(z, 1)] = tot[pl.ds(z, 1)]

    for t in range(T):
        for k, ref in enumerate((s1, s2, s3, s4)):
            for c in range(2):
                waiter(ref.at[t, c, pl.ds(0, n - 1)], ssem.at[k, t, c], rsem.at[k, t, c]).wait_send()
        table_done(t, True)
    for v in range(chips):
        waiter(pre.at[v], pssem.at[v], prsem.at[v]).wait_send()

    waiter(rq.at[pl.ds(0, chips - 1)], qssem, qrsem).wait_recv()
    for t in range(T):
        total = rq[0, t]
        for i in range(1, chips):
            total = total + rq[i, t]
        marg[t] = total * (1.0 / n)

    waiter(tot.at[pl.ds(0, chips - 1)], qssem, qrsem).wait_send()


def put_out(state, marg, state_out, marg_out, sem):
    copies = [
        pltpu.make_async_copy(src, dst, sem.at[k]) for k, (src, dst) in enumerate(((state, state_out), (marg, marg_out)))
    ]
    for copy in copies:
        copy.start()
    for copy in copies:
        copy.wait()


def on_device(n, wave_parts, level_table, phase_angles, mix_angles):
    wave = wave_parts.reshape(2, T, n, SUB, LANES)
    table = level_table.reshape(T, n, SUB, LANES)
    vmem, hbm = pl.BlockSpec(memory_space=pltpu.VMEM), pl.BlockSpec(memory_space=pltpu.HBM)
    state = pltpu.VMEM((T, 2, n, SUB, LANES), F32)
    half = pltpu.VMEM((T, n, SUB, LANES), F32)
    def share(count):
        return pltpu.VMEM((count, T, SUB, LANES), F32)

    dma = pltpu.SemaphoreType.DMA
    out, marg = pl.pallas_call(
        functools.partial(kernel, n),
        name="register",
        out_shape=(
            jax.ShapeDtypeStruct((2, T, n, SUB, LANES), F32),
            jax.ShapeDtypeStruct((T, SUB, LANES), F32),
        ),
        in_specs=[hbm] * 4,
        out_specs=(vmem, vmem),
        scratch_shapes=[
            pltpu.VMEM(wave.shape, F32),
            half,
            pltpu.VMEM(phase_angles.shape, F32),
            pltpu.VMEM(mix_angles.shape, F32),
        ]
        + [state] * 9
        + [share(n)]
        + [share(n // 2)] * 3
        + [half] * 3
        + [pltpu.VMEM((4, 2, LANES, LANES), jnp.bfloat16)]
        + [pltpu.SemaphoreType.REGULAR, dma((4,)), dma((4, T, 2)), dma((4, T, 2)), dma((T,)), dma((T,))]
        + [dma((n // 2,)), dma((n // 2,)), dma, dma],
        compiler_params=pltpu.CompilerParams(
            collective_id=0, has_side_effects=True, vmem_limit_bytes=24 * 1024 * 1024
        ),
    )(*(pltpu.with_memory_space_constraint(x, pltpu.HBM) for x in (wave, table, phase_angles, mix_angles)))
    out, marg = pl.pallas_call(
        put_out,
        name="put_out",
        out_shape=(jax.ShapeDtypeStruct(out.shape, F32), jax.ShapeDtypeStruct(marg.shape, F32)),
        in_specs=[vmem] * 2,
        out_specs=(hbm, hbm),
        scratch_shapes=[dma((2,))],
        compiler_params=pltpu.CompilerParams(vmem_limit_bytes=8 * 1024 * 1024),
    )(out, marg)
    return out.reshape(wave_parts.shape), marg


def solution(mesh):
    n = mesh.shape["high"]
    in_specs = (P(None, ("high", "low"), None, None), P(("high", "low"), None, None), P(), P())
    out_specs = (P(None, ("high", "low"), None, None), P("low", "high", None))
    return jax.shard_map(
        functools.partial(on_device, n), mesh=mesh, in_specs=in_specs, out_specs=out_specs, check_vma=False
    )
```
